128 devices in a mesh: strip: 32 (over z, y_lo, x), wave: 4 (over y_hi, core).
Axes of the slice: x: 4, y: 4 (y_hi: 2, y_lo: 2; y = y_hi * 2 + y_lo), z: 4, core: 2. Of those that a mesh axis runs over, the one named last changes fastest.
Arguments:
- source: bfloat16 [64, 1024, 2, 512], P('strip', None, None, 'wave'), parts along dimension 3, may hold values from -4 to 4
- pivot_inverse_real: bfloat16 [64, 4096, 1024], P('strip', 'wave'), parts along dimension 1, may hold values from -1 to 1
- factor_imag: bfloat16 [64, 4096, 1024], P('strip', 'wave'), parts along dimension 1, may hold values from -1 to 1
Outputs:
- solution: bfloat16 [64, 1024, 2, 512], P('strip', None, None, 'wave'), parts along dimension 3
The draws below stay inside these ranges and needn't reach their ends.
There are 4 independent parts, one for each index of `wave`. The reference program is written for one: setup_inputs(seed, part) draws one part's arguments, and reference() takes and returns one part's arrays. A program takes and returns all parts, laid end to end along the dimension named above; each array names one. Nothing has to cross between parts.
All inputs are finite; a program needn't handle non-finite values.
Results may differ from the reference program's by a relative error of at most 0.033.
Values may be sent and summed in bfloat16 or wider, within the bound.
No kernel may reach another device: no remote copies, remote signals or barrier semaphores. Data moves between devices by JAX's collectives and lax.ppermute only.
A program may use at most 64 MiB of HBM per device.

```python
import jax
import jax.numpy as jnp
from jax import lax

NY = 1024
RHS = 128
LAYER_TOTAL = 64


def factor_parts(key):
    draw_keys = jax.random.split(jax.random.fold_in(key, 31), 8)
    slow_share = 0.5
    slow_mode = jax.random.bernoulli(draw_keys[0], slow_share, (NY,))
    spread = jnp.exp(jax.random.uniform(draw_keys[1], (LAYER_TOTAL, NY), jnp.float32, -0.7, 0.7))
    fast_rate = jnp.exp(jax.random.uniform(draw_keys[2], (NY,), jnp.float32, jnp.log(1.0 / 20.0), jnp.log(1.0 / 8.0)))
    attenuation_factor = jnp.where(slow_mode, 1.0 / LAYER_TOTAL, fast_rate)[None, :] * spread
    surge_events = jax.random.bernoulli(draw_keys[3], 3.0 / LAYER_TOTAL, (LAYER_TOTAL, 1))
    surge_damping = jax.random.uniform(draw_keys[4], (LAYER_TOTAL, 1), jnp.float32, 0.5, 0.8)
    amplitude_level = 0.98 * jnp.exp(-attenuation_factor) * jnp.where(surge_events, surge_damping, 1.0)
    phases = jax.random.uniform(draw_keys[5], (LAYER_TOTAL, NY), jnp.float32, -jnp.pi, jnp.pi)
    mixing = 0.2 / jnp.sqrt(2.0 * NY)
    identity = jnp.eye(NY, dtype=jnp.float32)
    off_diagonal = 1.0 - identity
    real_noise = jnp.clip(jax.random.normal(draw_keys[6], (LAYER_TOTAL, NY, NY), jnp.float32), -6.0, 6.0)
    imag_noise = jnp.clip(jax.random.normal(draw_keys[7], (LAYER_TOTAL, NY, NY), jnp.float32), -6.0, 6.0)
    real_part = real_noise * mixing * off_diagonal + identity[None] * (amplitude_level * jnp.cos(phases))[:, None, :]
    imag_part = imag_noise * mixing * off_diagonal + identity[None] * (amplitude_level * jnp.sin(phases))[:, None, :]
    return (real_part, imag_part)


def draw_pivot_inverse_real(key, part):
    real_part, imag_part = factor_parts(key)
    return real_part.astype(jnp.bfloat16)


def draw_factor_imag(key, part):
    real_part, imag_part = factor_parts(key)
    return imag_part.astype(jnp.bfloat16)


def steps_of(stream_key, dims, cuts, low, largest):
    def one(dim, parts):
        heights = jax.random.uniform(jax.random.fold_in(jax.random.fold_in(stream_key, 6), dim), (parts,), jnp.float32, low / len(cuts), largest / len(cuts))
        return jnp.repeat(jnp.exp(heights), dims[dim] // parts).reshape((-1,) + (1,) * (len(dims) - dim - 1))

    factor_of = one(*cuts[0])
    for cut in cuts[1:]:
        factor_of = factor_of * one(*cut)
    return factor_of


def scatter_about(rng, extent, deviation, reach, cuts=(), held_as=jnp.bfloat16):
    loudness = steps_of(rng, extent, cuts, -0.22, 0.18) if cuts else 1.0
    array = jax.random.normal(rng, extent, jnp.float32) * deviation * loudness
    return jnp.minimum(jnp.maximum(array, -reach), reach).astype(held_as)


def setup_inputs(seed: int = 0, part: int = 0) -> dict:
    streams_of = jax.random.split(jax.random.key(seed), 4)
    part_keys = jax.random.split(jax.random.fold_in(streams_of[3], part), 4)
    source = scatter_about(part_keys[0], (LAYER_TOTAL, NY, 2, RHS), 0.25, 4.0, ((0, 32),))
    pivot_inverse_real = draw_pivot_inverse_real(jax.random.fold_in(jax.random.fold_in(streams_of[3], part), 71), part)
    factor_imag = draw_factor_imag(jax.random.fold_in(jax.random.fold_in(streams_of[3], part), 71), part)
    return {"source": source, "pivot_inverse_real": pivot_inverse_real, "factor_imag": factor_imag}


def complex_apply(real_part, imag_part, vector):
    mode_count, halves, columns = vector.shape
    merged = vector.reshape(mode_count, halves * columns)
    direct = jnp.dot(real_part, merged, preferred_element_type=jnp.float32).reshape(mode_count, halves, columns)
    crossed = jnp.dot(imag_part, merged, preferred_element_type=jnp.float32).reshape(mode_count, halves, columns)
    return jnp.stack([direct[:, 0] - crossed[:, 1], direct[:, 1] + crossed[:, 0]], axis=1)


def reference(source, pivot_inverse_real, factor_imag):
    def forward(trace_before, inputs):
        layer_source, real_part, imag_part = inputs
        summed = (layer_source.astype(jnp.float32) + trace_before).astype(jnp.bfloat16)
        trace_after = complex_apply(real_part, imag_part, summed)
        return trace_after, trace_after

    initial = jnp.zeros(source.shape[1:], jnp.float32)
    unused, traces = lax.scan(forward, initial, (source, pivot_inverse_real, factor_imag))

    def backward(updated_field, inputs):
        trace_here, real_part, imag_part = inputs
        field_now = trace_here + complex_apply(real_part, imag_part, updated_field.astype(jnp.bfloat16))
        return field_now, field_now

    unused, fields = lax.scan(backward, initial, (traces, pivot_inverse_real, factor_imag), reverse=True)
    return fields.astype(jnp.bfloat16)
```

```python
import functools

import jax
import jax.numpy as jnp
from jax import lax
from jax.experimental import pallas as pl
from jax.experimental.pallas import tpu as pltpu
from jax.sharding import PartitionSpec as P

GROUP = 4
BATCHES = 4
CHUNK = 64
LAG = 2
AXIS = "strip"
BF16 = jnp.bfloat16
F32 = jnp.float32
MIB = 2**20

VMEM = pl.BlockSpec(memory_space=pltpu.VMEM)
SMEM = pl.BlockSpec(memory_space=pltpu.SMEM)
ANY = pl.BlockSpec(memory_space=pl.ANY)


def multiply(rows, matrix):
    real, imag = rows[0], rows[1]
    size = real.shape[-1]
    direct = jnp.concatenate([real, imag], axis=0)
    crossed = jnp.concatenate([-imag, real], axis=0)
    return jnp.dot(direct, matrix[0, :size, :], preferred_element_type=F32) + jnp.dot(
        crossed, matrix[1, :size, :], preferred_element_type=F32
    )


def halves(value):
    return value.reshape(2, value.shape[0] // 2, value.shape[1])


def call(kernel, outs, specs_in, specs_out, *operands, scratch=(), aliases=None, rows=32, times=1, limit=24):
    size = 1024
    return pl.pallas_call(
        kernel,
        out_shape=outs,
        in_specs=specs_in,
        out_specs=specs_out,
        scratch_shapes=scratch,
        input_output_aliases=aliases or {},
        compiler_params=pltpu.CompilerParams(vmem_limit_bytes=limit * MIB),
        cost_estimate=pl.CostEstimate(
            flops=8 * times * rows * size * size, bytes_accessed=4 * times * size * size, transcendentals=0
        ),
    )(*operands)


def sweep_kernel(aliased, flags, block, first, second, add_first, add_second, *refs):
    own, got, out, work, sems = refs[2:] if aliased else refs
    mode, row, extra = flags[0], flags[1], flags[2]
    chunk = block.shape[1]

    @pl.when(mode == 1)
    def _():
        for part in range(2):
            work[part] = first[part, pl.ds(pl.multiple_of(row, chunk), chunk), :]

    @pl.when(mode == 2)
    def _():
        place = pl.ds(pl.multiple_of(extra, chunk), chunk)
        entered = (block[...].astype(F32) + add_first[:, place, :].astype(F32)).astype(BF16)
        work[...] = (halves(multiply(entered, first)) + add_second[:, place, :].astype(F32)).astype(BF16)

    @pl.when(mode > 0)
    def _():
        place = pl.ds(pl.multiple_of(row, chunk), chunk)
        keep = pltpu.make_async_copy(block, got.at[:, place, :], sems.at[0])
        keep.start()
        out[...] = halves(multiply(work[...], second)).astype(BF16)
        store = pltpu.make_async_copy(out, own.at[:, place, :], sems.at[1])
        store.start()
        keep.wait()
        store.wait()


def sweep(flags, block, first, second, add_first, add_second, kept):
    chunk, size = block.shape[1:]
    length = size + add_first.shape[1] - chunk
    buffer = jax.ShapeDtypeStruct((2, length, size), BF16)
    return call(
        functools.partial(sweep_kernel, kept is not None),
        (buffer, buffer, jax.ShapeDtypeStruct(block.shape, BF16)),
        [SMEM] + [VMEM] * 5 + ([ANY, ANY] if kept else []),
        (ANY, ANY, VMEM),
        flags,
        block,
        first,
        second,
        add_first,
        add_second,
        *(kept or ()),
        scratch=[pltpu.VMEM(block.shape, BF16), pltpu.SemaphoreType.DMA((2,))],
        aliases={6: 0, 7: 1} if kept else None,
        rows=chunk,
        times=2,
    )


def chain_kernel(block, matrix, constant, out):
    out[...] = (halves(multiply(block[...], matrix)) + constant[...].astype(F32)).astype(BF16)


def chain(block, matrix, constant):
    return call(
        chain_kernel, jax.ShapeDtypeStruct(block.shape, BF16), [VMEM] * 3, VMEM, block, matrix, constant
    )


def trace_kernel(flags, entry, before, source, first, second, trace_first, trace_second, enter):
    size = entry.shape[2]

    @pl.when(flags[0] == 0)
    def _():
        enter[...] = entry[...].astype(F32)

    @pl.when(flags[0] != 0)
    def _():
        enter[...] = halves(multiply(entry[...], before)) + before[:, size:, :].astype(F32)

    one = halves(multiply((source[0].astype(F32) + enter[...]).astype(BF16), first))
    trace_first[...] = one
    trace_second[...] = halves(multiply((source[1].astype(F32) + one).astype(BF16), second))


def inner_kernel(block, first, second, trace_first, trace_second, out):
    middle = (trace_second[...] + halves(multiply(block[...], second))).astype(BF16)
    out[...] = (trace_first[...] + halves(multiply(middle, first))).astype(BF16)


def field_kernel(flags, entry, after, constant, first, second, trace_first, trace_second, out, enter):
    @pl.when(flags[0] == 0)
    def _():
        enter[...] = entry[...]

    @pl.when(flags[0] != 0)
    def _():
        enter[...] = (halves(multiply(entry[...], after)) + constant[...].astype(F32)).astype(BF16)

    field = (trace_second[...] + halves(multiply(enter[...], second))).astype(BF16)
    out[1] = field
    out[0] = (trace_first[...] + halves(multiply(field, first))).astype(BF16)


def take(buffer, index):
    return lax.dynamic_index_in_dim(buffer, index, 0, keepdims=False)


def put(buffer, value, index):
    return lax.dynamic_update_index_in_dim(buffer, value, index, 0)


def slot(index, count):
    return jnp.where(jnp.logical_and(index >= 0, index < count), index, count)


def shards(source, pivot_inverse_real, factor_imag):
    strips = lax.axis_size(AXIS)
    groups = strips // GROUP
    position = lax.axis_index(AXIS)
    group = position // GROUP
    place = position % GROUP
    mirror = GROUP - 1 - place
    size = source.shape[1]
    columns = source.shape[3]
    width = columns // BATCHES
    chunks = size // CHUNK
    total = (size + columns) // CHUNK

    vectors = source.transpose(0, 2, 3, 1)
    first, second = (
        jnp.stack([pivot_inverse_real[layer].T, factor_imag[layer].T]) for layer in range(2)
    )

    add_first, add_second = (jnp.pad(vectors[layer], ((0, 0), (CHUNK, 0), (0, 0))) for layer in range(2))
    nothing = jnp.zeros((2, CHUNK, size), BF16)
    up = [(s, s + 1) for s in range(strips) if s % GROUP != GROUP - 1]
    down = [(s + 1, s) for s, _ in up]

    def moved(outs, step, pairs, count):
        live = [
            (s, d)
            for s, d in pairs
            if 0 <= step - LAG * (s % GROUP if d > s else GROUP - 1 - s % GROUP) < count
        ]
        return lax.ppermute(outs[step - LAG], AXIS, live)

    def flags_of(step, rank, count):
        index = step - LAG * (rank - 1)
        valid = jnp.logical_and(index >= 0, index < count)
        mode = jnp.where(jnp.logical_and(rank == 0, index < chunks), 1, 2)
        return jnp.stack(
            [
                jnp.where(valid, mode, 0),
                jnp.clip(index, 0, count - 1) * CHUNK,
                jnp.clip(index - chunks + 1, 0, total - chunks) * CHUNK,
            ]
        ).astype(jnp.int32)

    outs_f, outs_b = {}, {}
    kept_f = kept_b = None
    for step in range(-LAG, total + LAG * (GROUP - 2)):
        block = moved(outs_f, step, up, total) if step >= 0 else nothing
        *kept_f, outs_f[step] = sweep(
            flags_of(step, place, total), block, first, second, add_first, add_second, kept_f
        )
        if step < chunks + LAG * (GROUP - 2):
            block = moved(outs_b, step, down, chunks) if step >= 0 else nothing
            *kept_b, outs_b[step] = sweep(
                flags_of(step, mirror, chunks), block, second, first, nothing, nothing, kept_b
            )
    prefix, prefix_before = kept_f
    suffix, suffix_after = kept_b

    def joined(value):
        return value[:BATCHES].swapaxes(0, 1).reshape(2, columns, size)

    nought = jnp.zeros((2, width, size), BF16)
    blocks = jnp.zeros((BATCHES + 1, 2, width, size), BF16)
    incoming = sent = blocks
    block = nought
    for moment in range(groups - 2 + BATCHES):
        index = slot(moment - group, BATCHES)
        start = size + jnp.minimum(index, BATCHES - 1) * width
        constant = lax.dynamic_slice_in_dim(prefix, start, width, 1)
        outgoing = chain(block, prefix, constant)
        sent = put(sent, outgoing, index)
        pairs = [
            (GROUP * g + GROUP - 1, GROUP * g + 2 * GROUP - 1)
            for g in range(groups - 1)
            if 0 <= moment - g < BATCHES
        ]
        block = lax.ppermute(outgoing, AXIS, pairs)
        incoming = put(incoming, block, slot(moment - group + 1, BATCHES))
    whole = joined(sent)
    entry = jnp.where(jnp.logical_and(place == GROUP - 1, group > 0), joined(incoming), 0)
    for other in range(GROUP - 1):
        entry += lax.ppermute(
            whole,
            AXIS,
            [(GROUP * g + GROUP - 1, GROUP * g + GROUP + other) for g in range(groups - 1)],
        )

    trace = jax.ShapeDtypeStruct((2, columns, size), F32)
    trace_first, trace_second = call(
        trace_kernel,
        (trace, trace),
        [SMEM] + [VMEM] * 5,
        (VMEM, VMEM),
        place[None].astype(jnp.int32),
        entry,
        prefix_before,
        vectors,
        first,
        second,
        scratch=[pltpu.VMEM((2, columns, size), F32)],
        rows=columns,
        times=3,
        limit=32,
    )

    inner = inner_sent = blocks
    block = nought
    for moment in range(GROUP - 1 + BATCHES):
        index = slot(moment - mirror, BATCHES)
        start = jnp.minimum(index, BATCHES - 1) * width
        outgoing = call(
            inner_kernel,
            jax.ShapeDtypeStruct(block.shape, BF16),
            [VMEM] * 5,
            VMEM,
            block,
            first,
            second,
            lax.dynamic_slice_in_dim(trace_first, start, width, 1),
            lax.dynamic_slice_in_dim(trace_second, start, width, 1),
            times=2,
        )
        inner_sent = put(inner_sent, outgoing, index)
        pairs = [(s, d) for s, d in down if 0 <= moment - (GROUP - 1 - s % GROUP) < BATCHES]
        if pairs:
            block = lax.ppermute(outgoing, AXIS, pairs)
            inner = put(inner, block, slot(moment - mirror + 1, BATCHES))
    incoming = sent = blocks
    block = nought
    far = groups - 1 - group
    for moment in range(groups - 2 + BATCHES):
        index = slot(moment - far, BATCHES)
        outgoing = chain(block, suffix, take(inner_sent, index))
        sent = put(sent, outgoing, index)
        pairs = [
            (GROUP * g + GROUP, GROUP * g)
            for g in range(groups - 1)
            if 0 <= moment - (groups - 2 - g) < BATCHES
        ]
        block = lax.ppermute(outgoing, AXIS, pairs)
        incoming = put(incoming, block, slot(moment - far + 1, BATCHES))
    whole = joined(sent)
    entry = jnp.where(jnp.logical_and(place == 0, far > 0), joined(incoming), 0)
    for other in range(1, GROUP):
        entry += lax.ppermute(
            whole, AXIS, [(GROUP * g + GROUP, GROUP * g + other) for g in range(groups - 1)]
        )
    fields = call(
        field_kernel,
        jax.ShapeDtypeStruct((2, 2, columns, size), BF16),
        [SMEM] + [VMEM] * 7,
        VMEM,
        mirror[None].astype(jnp.int32),
        entry,
        suffix_after,
        joined(inner),
        first,
        second,
        trace_first,
        trace_second,
        scratch=[pltpu.VMEM((2, columns, size), BF16)],
        rows=columns,
        times=3,
        limit=32,
    )
    return fields.transpose(0, 3, 1, 2)


def solution(mesh):
    placed = (P("strip", None, None, "wave"), P("strip", "wave", None), P("strip", "wave", None))
    return jax.shard_map(
        shards,
        mesh=mesh,
        in_specs=placed,
        out_specs=P("strip", None, None, "wave"),
        check_vma=False,
    )
```

```python
import functools

import jax
import jax.numpy as jnp
from jax import lax
from jax.experimental import pallas as pl
from jax.experimental.pallas import tpu as pltpu
from jax.sharding import PartitionSpec as P

GROUP = 4
BATCHES = 4
LAG = 2
AXIS = "strip"
BF16 = jnp.bfloat16
F32 = jnp.float32
MIB = 2**20

VMEM = pl.BlockSpec(memory_space=pltpu.VMEM)
SMEM = pl.BlockSpec(memory_space=pltpu.SMEM)
ANY = pl.BlockSpec(memory_space=pl.ANY)
PLAIN = (((1,), (0,)), ((), ()))
TURNED = (((1,), (1,)), ((), ()))


def resident(value):
    return pltpu.with_memory_space_constraint(value, pltpu.VMEM)


def held(*shape, dtype=BF16):
    return pltpu.VMEM(shape, dtype)


def whole(value):
    return jax.ShapeDtypeStruct(value.shape, value.dtype)


def call(kernel, outs, operands, specs, scratch=(), aliases=None, rows=32, times=1, limit=12):
    size = 1024
    return pl.pallas_call(
        kernel,
        out_shape=outs,
        in_specs=specs,
        out_specs=jax.tree.map(lambda _: VMEM, outs),
        scratch_shapes=scratch,
        input_output_aliases=aliases or {},
        compiler_params=pltpu.CompilerParams(vmem_limit_bytes=limit * MIB),
        cost_estimate=pl.CostEstimate(
            flops=8 * times * rows * size * size, bytes_accessed=4 * times * size * size, transcendentals=0
        ),
    )(*operands)


def product(direct, crossed, real, imag, out, tile, turned):
    dims = TURNED if turned else PLAIN
    tile = min(tile, real.shape[0])

    def body(step, carry):
        columns = pl.ds(pl.multiple_of(step * tile, tile), tile)
        where = (columns, slice(None)) if turned else (slice(None), columns)
        out(
            columns,
            lax.dot_general(direct[...], real[where], dims, preferred_element_type=F32)
            + lax.dot_general(crossed[...], imag[where], dims, preferred_element_type=F32),
        )
        return carry

    lax.fori_loop(0, real.shape[0] // tile, body, 0)


def spread(rows, direct, crossed):
    count = direct.shape[0] // 2
    direct[:count] = rows[0]
    direct[count:] = rows[1]
    crossed[:count] = -rows[1]
    crossed[count:] = rows[0]


def halves(value):
    return value.reshape(2, value.shape[0] // 2, value.shape[1])


def stage_kernel(real, imag, real_out, imag_out, sems):
    copies = [
        pltpu.make_async_copy(real, real_out, sems.at[0]),
        pltpu.make_async_copy(imag, imag_out, sems.at[1]),
    ]
    for copy in copies:
        copy.start()
    for copy in copies:
        copy.wait()


def between(index, count):
    return jnp.logical_and(index >= 0, index < count)


def sweep_kernel(step, aliased, place_ref, block_f, block_b, real, imag, source, *refs):
    own_f, got_f, own_b, got_b, out_f, out_b, direct, crossed, result = refs[4:] if aliased else refs
    chunk, size = block_f.shape[1:]
    chunks = size // chunk
    place = place_ref[0]
    index_f = step - LAG * (place - 1)
    index_b = step - LAG * (GROUP - 2 - place)
    last = index_f == chunks
    active_f, active_b = between(index_f, chunks + 1), between(index_b, chunks)
    row_f, row_b = (jnp.clip(index, 0, chunks) * chunk for index in (index_f, index_b))

    for way, (block, row, active, starts) in enumerate(
        (
            (block_f, row_f, active_f, jnp.logical_and(place == 0, jnp.logical_not(last))),
            (block_b, row_b, active_b, place == GROUP - 1),
        )
    ):

        @pl.when(jnp.logical_and(active, starts))
        def _(way=way, row=row):
            shape = (chunk, size)
            hit = lax.broadcasted_iota(jnp.int32, shape, 1) == lax.broadcasted_iota(jnp.int32, shape, 0) + row
            one = jnp.where(hit, 1.0, 0.0).astype(BF16)
            spread((one, jnp.zeros(shape, BF16)), direct.at[way], crossed.at[way])

        @pl.when(jnp.logical_and(active, jnp.logical_not(starts)))
        def _(way=way, block=block):
            spread(block, direct.at[way], crossed.at[way])

    @pl.when(last)
    def _():
        entered = (block_f[...].astype(F32) + source[0].astype(F32)).astype(BF16)
        spread(entered, direct.at[0], crossed.at[0])

    def multiply(way, layer):
        def keep(columns, value):
            result[way, :, :, columns] = halves(value)

        product(
            direct.at[way], crossed.at[way], real.at[layer], imag.at[layer], keep, 256, True
        )

    def both(way, carry):
        @pl.when(jnp.logical_or(jnp.logical_and(way == 0, active_f), jnp.logical_and(way == 1, active_b)))
        def _():
            multiply(way, way)

            @pl.when(jnp.logical_and(way == 0, last))
            def _():
                result[way] += source[1].astype(F32)

            spread(result[way].astype(BF16), direct.at[way], crossed.at[way])
            multiply(way, 1 - way)

        return carry

    lax.fori_loop(0, 2, both, 0)
    for way, (block, own, got, out, row, active) in enumerate(
        (
            (block_f, own_f, got_f, out_f, row_f, active_f),
            (block_b, own_b, got_b, out_b, row_b, active_b),
        )
    ):

        @pl.when(active)
        def _(way=way, row=row, block=block, own=own, got=got, out=out):
            rows = pl.ds(pl.multiple_of(row, chunk), chunk)
            done = result[way].astype(BF16)
            out[...] = done
            own[:, rows, :] = done
            got[:, rows, :] = block[...]


def sweep(step, place, block_f, block_b, real, imag, source, kept):
    _, chunk, size = block_f.shape
    outs = [whole(value) for value in kept] or [
        held(2, length, size) for length in (size + chunk,) * 2 + (size,) * 2
    ]
    return call(
        functools.partial(sweep_kernel, step, bool(kept)),
        (*outs, whole(block_f), whole(block_b)),
        (place, block_f, block_b, resident(real), resident(imag), resident(source), *map(resident, kept)),
        [SMEM] + [VMEM] * (5 + len(kept)),
        scratch=[
            pltpu.VMEM((2, 2 * chunk, size), BF16),
            pltpu.VMEM((2, 2 * chunk, size), BF16),
            pltpu.VMEM((2, 2, chunk, size), F32),
        ],
        aliases={6 + i: i for i in range(4)} if kept else None,
        rows=chunk,
        times=4,
    )


def stacked(count, size):
    return [pltpu.VMEM((2 * count, size), BF16)] * 2


def chain_kernel(moment, spread_from, inward, aliased, place_ref, block, matrix, constants, *refs):
    refs = refs[2:] if aliased else refs
    sent, came, out, copy, direct, crossed = refs
    size = block.shape[2]
    width = block.shape[1]
    place, group, far = place_ref[0], place_ref[1], place_ref[2]
    batch = moment - (far if inward else group)
    node = jnp.logical_and(place == (0 if inward else GROUP - 1), between(batch, BATCHES))
    sends = jnp.logical_and(node, (group if inward else far) > 0)
    index = jnp.clip(batch, 0, BATCHES - 1)

    @pl.when(node)
    def _():
        came[index] = block[...]

    @pl.when(sends)
    def _():
        spread(block, direct, crossed)

        def keep(columns, value):
            if inward:
                constant = constants[index, :, :, columns]
            else:
                constant = matrix[:, pl.ds(pl.multiple_of(size + index * width, width), width), columns]
            out[:, :, columns] = (halves(value) + constant.astype(F32)).astype(BF16)

        product(direct, crossed, matrix.at[0, :size], matrix.at[1, :size], keep, 512, False)
        sent[index] = out[...]

    if 0 <= moment - spread_from < BATCHES:
        copy[...] = sent[moment - spread_from]


def chain(moment, spread_from, inward, place, block, matrix, constants, kept):
    outs = [whole(value) for value in kept] or [held(BATCHES, *block.shape)] * 2
    *kept, out, copy = call(
        functools.partial(chain_kernel, moment, spread_from, inward, bool(kept)),
        (*outs, whole(block), whole(block)),
        (place, block, resident(matrix), resident(constants), *map(resident, kept)),
        [SMEM] + [VMEM] * (3 + len(kept)),
        scratch=stacked(*block.shape[1:]),
        aliases={4: 0, 5: 1} if kept else None,
    )
    return kept, out, copy


def pick_entry(place, mine, entries, came, batch, direct, crossed):
    @pl.when(place == mine)
    def _():
        spread(came.at[batch], direct, crossed)

    others = [other for other in range(GROUP) if other != mine]
    for other, entry in zip(others, entries):

        @pl.when(place == other)
        def _(entry=entry):
            spread(entry, direct, crossed)


def trace_kernel(batch, aliased, place_ref, *refs):
    *entries, came, before, source, real, imag = refs[: GROUP + 4]
    refs = refs[GROUP + 4 :]
    trace_first, trace_second, enter, direct, crossed = refs[2:] if aliased else refs
    size, width = before.shape[2], enter.shape[1]
    place = place_ref[0]
    rows = pl.ds(batch * width, width)
    pick_entry(place, GROUP - 1, entries, came, batch, direct, crossed)

    @pl.when(place == 0)
    def _():
        enter[...] = entries[0][...].astype(F32)

    @pl.when(place != 0)
    def _():
        def keep(columns, value):
            constant = before[:, pl.ds(size + batch * width, width), columns]
            enter[:, :, columns] = halves(value) + constant.astype(F32)

        product(direct, crossed, before.at[0, :size], before.at[1, :size], keep, 512, False)

    def keep_first(columns, value):
        trace_first[batch, :, :, columns] = halves(value)

    def keep_second(columns, value):
        trace_second[batch, :, :, columns] = halves(value)

    spread((source[0, :, rows, :].astype(F32) + enter[...]).astype(BF16), direct, crossed)
    product(direct, crossed, real.at[0], imag.at[0], keep_first, 512, True)
    spread((source[1, :, rows, :].astype(F32) + trace_first[batch]).astype(BF16), direct, crossed)
    product(direct, crossed, real.at[1], imag.at[1], keep_second, 512, True)


def inner_kernel(moment, aliased, place_ref, block, real, imag, trace_first, trace_second, *refs):
    sent, came, out, middle, direct, crossed = refs[2:] if aliased else refs
    mirror = GROUP - 1 - place_ref[0]
    batch = moment - mirror
    index = jnp.clip(batch, 0, BATCHES - 1)

    @pl.when(between(batch, BATCHES))
    def _():
        middle[...] = trace_second[index].astype(BF16)

        @pl.when(mirror != 0)
        def _():
            came[index] = block[...]
            spread(block, direct, crossed)

            def keep(columns, value):
                middle[:, :, columns] = (trace_second[index, :, :, columns] + halves(value)).astype(BF16)

            product(direct, crossed, real.at[1], imag.at[1], keep, 512, True)

        def keep_out(columns, value):
            out[:, :, columns] = (trace_first[index, :, :, columns] + halves(value)).astype(BF16)

        spread(middle, direct, crossed)
        product(direct, crossed, real.at[0], imag.at[0], keep_out, 512, True)
        sent[index] = out[...]


def field_kernel(batch, aliased, place_ref, *refs):
    *entries, came, after, constants, real, imag, trace_first, trace_second = refs[: GROUP + 6]
    refs = refs[GROUP + 6 :]
    out, enter, direct, crossed = refs[1:] if aliased else refs
    width = enter.shape[1]
    place = place_ref[0]
    rows = pl.ds(batch * width, width)
    pick_entry(place, 0, entries, came, batch, direct, crossed)

    @pl.when(place != GROUP - 1)
    def _():
        def keep(columns, value):
            enter[:, :, columns] = (halves(value) + constants[batch, :, :, columns].astype(F32)).astype(BF16)

        product(direct, crossed, after.at[0], after.at[1], keep, 512, False)
        spread(enter, direct, crossed)

    def keep_second(columns, value):
        enter[:, :, columns] = (trace_second[batch, :, :, columns] + halves(value)).astype(BF16)

    def keep_first(columns, value):
        out[0, :, rows, columns] = (trace_first[batch, :, :, columns] + halves(value)).astype(BF16)

    product(direct, crossed, real.at[1], imag.at[1], keep_second, 512, True)
    out[1, :, rows, :] = enter[...]
    spread(enter, direct, crossed)
    product(direct, crossed, real.at[0], imag.at[0], keep_first, 512, True)


def shards(source, pivot_inverse_real, factor_imag):
    strips = lax.axis_size(AXIS)
    groups = strips // GROUP
    position = lax.axis_index(AXIS)
    group = position // GROUP
    place = jnp.stack([position % GROUP, group, groups - 1 - group]).astype(jnp.int32)
    size = source.shape[1]
    columns = source.shape[3]
    width = columns // BATCHES
    chunk = columns
    chunks = size // chunk
    total = chunks + 1

    vectors = source.transpose(0, 2, 3, 1)
    real, imag = call(
        stage_kernel,
        tuple(held(*value.shape) for value in (pivot_inverse_real, factor_imag)),
        (pivot_inverse_real, factor_imag),
        [ANY, ANY],
        scratch=[pltpu.SemaphoreType.DMA((2,))],
    )

    nothing = jnp.zeros((2, chunk, size), BF16)
    up = [(s, s + 1) for s in range(strips) if s % GROUP != GROUP - 1]
    down = [(s + 1, s) for s, _ in up]

    def moved(outs, step, pairs, count):
        live = [
            (s, d)
            for s, d in pairs
            if 0 <= step - LAG * (s % GROUP if d > s else GROUP - 1 - s % GROUP) < count
        ]
        return lax.ppermute(outs[step - LAG], AXIS, live) if live and step >= 0 else nothing

    outs_f, outs_b = {}, {}
    kept = ()
    for step in range(-LAG, total + LAG * (GROUP - 2)):
        *kept, outs_f[step], outs_b[step] = sweep(
            step,
            place,
            moved(outs_f, step, up, total),
            moved(outs_b, step, down, chunks),
            real,
            imag,
            vectors,
            kept,
        )
    prefix, prefix_before, suffix, suffix_after = kept

    block = jax.ShapeDtypeStruct((2, width, size), BF16)
    nought = jnp.zeros((2, width, size), BF16)
    block_f = block_i = block_b = nought
    kept_f = kept_i = kept_b = traces = fields = ()
    spread_f, spread_b = {}, {}
    turn = groups - 2
    inner_start = turn + 1
    back_start = inner_start + GROUP - 1
    back_end = back_start + turn
    for moment in range(back_end + BATCHES + 1):
        if moment <= turn + BATCHES:
            kept_f, outgoing, copy = chain(
                moment, turn, False, place, block_f, prefix, vectors, kept_f
            )
            pairs = [
                (GROUP * g + GROUP - 1, GROUP * g + 2 * GROUP - 1)
                for g in range(groups - 1)
                if 0 <= moment - g < BATCHES
            ]
            if pairs:
                block_f = lax.ppermute(outgoing, AXIS, pairs)
            if 0 <= moment - turn < BATCHES:
                spread_f[moment - turn] = [
                    lax.ppermute(
                        copy,
                        AXIS,
                        [(GROUP * g + GROUP - 1, GROUP * g + GROUP + other) for g in range(groups - 1)],
                    )
                    for other in range(GROUP - 1)
                ]
        batch = moment - inner_start
        if 0 <= batch < BATCHES:
            outs = [whole(value) for value in traces] or [held(BATCHES, 2, width, size, dtype=F32)] * 2
            traces = call(
                functools.partial(trace_kernel, batch, bool(traces)),
                tuple(outs),
                (
                    place,
                    *spread_f[batch],
                    *map(resident, (kept_f[1], prefix_before, vectors, real, imag, *traces)),
                ),
                [SMEM] + [VMEM] * (GROUP + 4 + len(traces)),
                scratch=[pltpu.VMEM((2, width, size), F32)] + stacked(width, size),
                aliases={GROUP + 5: 0, GROUP + 6: 1} if traces else None,
                times=3,
            )
        if inner_start <= moment < back_start + BATCHES:
            outs = [whole(value) for value in kept_i] or [held(BATCHES, 2, width, size)] * 2
            *kept_i, outgoing = call(
                functools.partial(inner_kernel, moment - inner_start, bool(kept_i)),
                (*outs, block),
                (place, block_i, *map(resident, (real, imag, *traces, *kept_i))),
                [SMEM] + [VMEM] * (5 + len(kept_i)),
                scratch=[pltpu.VMEM((2, width, size), BF16)] + stacked(width, size),
                aliases={6: 0, 7: 1} if kept_i else None,
                times=2,
            )
            pairs = [
                (s, d)
                for s, d in down
                if 0 <= moment - inner_start - (GROUP - 1 - s % GROUP) < BATCHES
            ]
            if pairs:
                block_i = lax.ppermute(outgoing, AXIS, pairs)
        if back_start <= moment <= back_end + BATCHES:
            kept_b, outgoing, copy = chain(
                moment - back_start, turn, True, place, block_b, suffix, kept_i[0], kept_b
            )
            pairs = [
                (GROUP * g + GROUP, GROUP * g)
                for g in range(groups - 1)
                if 0 <= moment - back_start - (groups - 2 - g) < BATCHES
            ]
            if pairs:
                block_b = lax.ppermute(outgoing, AXIS, pairs)
            if 0 <= moment - back_end < BATCHES:
                spread_b[moment - back_end] = [
                    lax.ppermute(
                        copy,
                        AXIS,
                        [(GROUP * g + GROUP, GROUP * g + other) for g in range(groups - 1)],
                    )
                    for other in range(1, GROUP)
                ]
        batch = moment - back_end - 1
        if batch >= 0:
            fields = (
                call(
                    functools.partial(field_kernel, batch, bool(fields)),
                    whole(fields[0]) if fields else held(2, 2, columns, size),
                    (
                        place,
                        *spread_b[batch],
                        *map(
                            resident,
                            (kept_b[1], suffix_after, kept_i[1], real, imag, *traces, *fields),
                        ),
                    ),
                    [SMEM] + [VMEM] * (GROUP + 6 + len(fields)),
                    scratch=[pltpu.VMEM((2, width, size), BF16)] + stacked(width, size),
                    aliases={GROUP + 7: 0} if fields else None,
                    times=3,
                ),
            )
    return fields[0].transpose(0, 3, 1, 2)


def solution(mesh):
    placed = (P("strip", None, None, "wave"), P("strip", "wave", None), P("strip", "wave", None))
    return jax.shard_map(
        shards,
        mesh=mesh,
        in_specs=placed,
        out_specs=P("strip", None, None, "wave"),
        check_vma=False,
    )
```

```python
import functools

import jax
import jax.numpy as jnp
from jax import lax
from jax.experimental import pallas as pl
from jax.experimental.pallas import tpu as pltpu
from jax.sharding import PartitionSpec as P

GROUP = 4
BATCHES = 4
LAG = 2
AXIS = "strip"
BF16 = jnp.bfloat16
F32 = jnp.float32
MIB = 2**20

VMEM = pl.BlockSpec(memory_space=pltpu.VMEM)
SMEM = pl.BlockSpec(memory_space=pltpu.SMEM)
ANY = pl.BlockSpec(memory_space=pl.ANY)
PLAIN = (((1,), (0,)), ((), ()))
TURNED = (((1,), (1,)), ((), ()))


def resident(value):
    return pltpu.with_memory_space_constraint(value, pltpu.VMEM)


def held(*shape, dtype=BF16):
    return pltpu.VMEM(shape, dtype)


def whole(value):
    return jax.ShapeDtypeStruct(value.shape, value.dtype)


def call(kernel, outs, operands, specs, scratch=(), aliases=None, rows=32, times=1, limit=12):
    size = 1024
    return pl.pallas_call(
        kernel,
        out_shape=outs,
        in_specs=specs,
        out_specs=jax.tree.map(lambda _: VMEM, outs),
        scratch_shapes=scratch,
        input_output_aliases=aliases or {},
        compiler_params=pltpu.CompilerParams(vmem_limit_bytes=limit * MIB),
        cost_estimate=pl.CostEstimate(
            flops=8 * times * rows * size * size, bytes_accessed=4 * times * size * size, transcendentals=0
        ),
    )(*operands)


def product(direct, crossed, real, imag, out, tile, turned):
    dims = TURNED if turned else PLAIN
    tile = min(tile, real.shape[0])

    def body(step, carry):
        columns = pl.ds(pl.multiple_of(step * tile, tile), tile)
        where = (columns, slice(None)) if turned else (slice(None), columns)
        out(
            columns,
            lax.dot_general(direct[...], real[where], dims, preferred_element_type=F32)
            + lax.dot_general(crossed[...], imag[where], dims, preferred_element_type=F32),
        )
        return carry

    lax.fori_loop(0, real.shape[0] // tile, body, 0)


def spread(rows, direct, crossed):
    count = direct.shape[0] // 2
    direct[:count] = rows[0]
    direct[count:] = rows[1]
    crossed[:count] = -rows[1]
    crossed[count:] = rows[0]


def halves(value):
    return value.reshape(2, value.shape[0] // 2, value.shape[1])


def stage_kernel(real, imag, real_out, imag_out, sems):
    copies = [
        pltpu.make_async_copy(real, real_out, sems.at[0]),
        pltpu.make_async_copy(imag, imag_out, sems.at[1]),
    ]
    for copy in copies:
        copy.start()
    for copy in copies:
        copy.wait()


def between(index, count):
    return jnp.logical_and(index >= 0, index < count)


def sweep_kernel(step, aliased, place_ref, block_f, block_b, real, imag, source, *refs):
    own_f, got_f, own_b, got_b, out_f, out_b, direct, crossed, result = refs[4:] if aliased else refs
    chunk, size = block_f.shape[1:]
    chunks = size // chunk
    place = place_ref[0]
    index_f = step - LAG * (place - 1)
    index_b = step - LAG * (GROUP - 2 - place)
    last = index_f == chunks
    active_f, active_b = between(index_f, chunks + 1), between(index_b, chunks)
    row_f, row_b = (jnp.clip(index, 0, chunks) * chunk for index in (index_f, index_b))

    for way, (block, row, active, starts) in enumerate(
        (
            (block_f, row_f, active_f, jnp.logical_and(place == 0, jnp.logical_not(last))),
            (block_b, row_b, active_b, place == GROUP - 1),
        )
    ):

        @pl.when(jnp.logical_and(active, starts))
        def _(way=way, row=row):
            shape = (chunk, size)
            hit = lax.broadcasted_iota(jnp.int32, shape, 1) == lax.broadcasted_iota(jnp.int32, shape, 0) + row
            one = jnp.where(hit, 1.0, 0.0).astype(BF16)
            spread((one, jnp.zeros(shape, BF16)), direct.at[way], crossed.at[way])

        @pl.when(jnp.logical_and(active, jnp.logical_not(starts)))
        def _(way=way, block=block):
            spread(block, direct.at[way], crossed.at[way])

    @pl.when(last)
    def _():
        entered = (block_f[...].astype(F32) + source[0].astype(F32)).astype(BF16)
        spread(entered, direct.at[0], crossed.at[0])

    def multiply(way, layer):
        def keep(columns, value):
            result[way, :, :, columns] = halves(value)

        product(
            direct.at[way], crossed.at[way], real.at[layer], imag.at[layer], keep, 512, True
        )

    def both(way, carry):
        @pl.when(jnp.logical_or(jnp.logical_and(way == 0, active_f), jnp.logical_and(way == 1, active_b)))
        def _():
            multiply(way, way)

            @pl.when(jnp.logical_and(way == 0, last))
            def _():
                result[way] += source[1].astype(F32)

            spread(result[way].astype(BF16), direct.at[way], crossed.at[way])
            multiply(way, 1 - way)

        return carry

    lax.fori_loop(0, 2, both, 0)
    for way, (block, own, got, out, row, active) in enumerate(
        (
            (block_f, own_f, got_f, out_f, row_f, active_f),
            (block_b, own_b, got_b, out_b, row_b, active_b),
        )
    ):

        @pl.when(active)
        def _(way=way, row=row, block=block, own=own, got=got, out=out):
            rows = pl.ds(pl.multiple_of(row, chunk), chunk)
            done = result[way].astype(BF16)
            out[...] = done
            own[:, rows, :] = done
            got[:, rows, :] = block[...]


def sweep(step, place, block_f, block_b, real, imag, source, kept):
    _, chunk, size = block_f.shape
    outs = [whole(value) for value in kept] or [
        held(2, length, size) for length in (size + chunk,) * 2 + (size,) * 2
    ]
    return call(
        functools.partial(sweep_kernel, step, bool(kept)),
        (*outs, whole(block_f), whole(block_b)),
        (place, block_f, block_b, resident(real), resident(imag), resident(source), *map(resident, kept)),
        [SMEM] + [VMEM] * (5 + len(kept)),
        scratch=[
            pltpu.VMEM((2, 2 * chunk, size), BF16),
            pltpu.VMEM((2, 2 * chunk, size), BF16),
            pltpu.VMEM((2, 2, chunk, size), F32),
        ],
        aliases={6 + i: i for i in range(4)} if kept else None,
        rows=chunk,
        times=4,
    )


def stacked(count, size):
    return [pltpu.VMEM((2 * count, size), BF16)] * 2


def chain_kernel(moment, spread_from, inward, aliased, place_ref, block, matrix, constants, *refs):
    refs = refs[2:] if aliased else refs
    sent, came, out, copy, direct, crossed = refs
    size = block.shape[2]
    width = block.shape[1]
    place, group, far = place_ref[0], place_ref[1], place_ref[2]
    batch = moment - (far if inward else group)
    node = jnp.logical_and(place == (0 if inward else GROUP - 1), between(batch, BATCHES))
    sends = jnp.logical_and(node, (group if inward else far) > 0)
    index = jnp.clip(batch, 0, BATCHES - 1)

    @pl.when(node)
    def _():
        came[index] = block[...]

    @pl.when(sends)
    def _():
        spread(block, direct, crossed)

        def keep(columns, value):
            if inward:
                constant = constants[index, :, :, columns]
            else:
                constant = matrix[:, pl.ds(pl.multiple_of(size + index * width, width), width), columns]
            out[:, :, columns] = (halves(value) + constant.astype(F32)).astype(BF16)

        product(direct, crossed, matrix.at[0, :size], matrix.at[1, :size], keep, 512, False)
        sent[index] = out[...]

    if 0 <= moment - spread_from < BATCHES:
        copy[...] = sent[moment - spread_from]


def chain(moment, spread_from, inward, place, block, matrix, constants, kept):
    outs = [whole(value) for value in kept] or [held(BATCHES, *block.shape)] * 2
    *kept, out, copy = call(
        functools.partial(chain_kernel, moment, spread_from, inward, bool(kept)),
        (*outs, whole(block), whole(block)),
        (place, block, resident(matrix), resident(constants), *map(resident, kept)),
        [SMEM] + [VMEM] * (3 + len(kept)),
        scratch=stacked(*block.shape[1:]),
        aliases={4: 0, 5: 1} if kept else None,
    )
    return kept, out, copy


def pick_entry(place, mine, entries, came, batch, direct, crossed):
    @pl.when(place == mine)
    def _():
        spread(came.at[batch], direct, crossed)

    others = [other for other in range(GROUP) if other != mine]
    for other, entry in zip(others, entries):

        @pl.when(place == other)
        def _(entry=entry):
            spread(entry, direct, crossed)


def trace_kernel(batch, aliased, place_ref, *refs):
    *entries, came, before, source, real, imag = refs[: GROUP + 4]
    refs = refs[GROUP + 4 :]
    trace_first, trace_second, enter, direct, crossed = refs[2:] if aliased else refs
    size, width = before.shape[2], enter.shape[1]
    place = place_ref[0]
    rows = pl.ds(batch * width, width)
    pick_entry(place, GROUP - 1, entries, came, batch, direct, crossed)

    @pl.when(place == 0)
    def _():
        enter[...] = entries[0][...].astype(F32)

    @pl.when(place != 0)
    def _():
        def keep(columns, value):
            constant = before[:, pl.ds(size + batch * width, width), columns]
            enter[:, :, columns] = halves(value) + constant.astype(F32)

        product(direct, crossed, before.at[0, :size], before.at[1, :size], keep, 512, False)

    def keep_first(columns, value):
        trace_first[batch, :, :, columns] = halves(value)

    def keep_second(columns, value):
        trace_second[batch, :, :, columns] = halves(value)

    spread((source[0, :, rows, :].astype(F32) + enter[...]).astype(BF16), direct, crossed)
    product(direct, crossed, real.at[0], imag.at[0], keep_first, 512, True)
    spread((source[1, :, rows, :].astype(F32) + trace_first[batch]).astype(BF16), direct, crossed)
    product(direct, crossed, real.at[1], imag.at[1], keep_second, 512, True)


def inner_kernel(moment, aliased, place_ref, block, real, imag, trace_first, trace_second, *refs):
    sent, came, out, middle, direct, crossed = refs[2:] if aliased else refs
    mirror = GROUP - 1 - place_ref[0]
    batch = moment - mirror
    index = jnp.clip(batch, 0, BATCHES - 1)

    @pl.when(between(batch, BATCHES))
    def _():
        middle[...] = trace_second[index].astype(BF16)

        @pl.when(mirror != 0)
        def _():
            came[index] = block[...]
            spread(block, direct, crossed)

            def keep(columns, value):
                middle[:, :, columns] = (trace_second[index, :, :, columns] + halves(value)).astype(BF16)

            product(direct, crossed, real.at[1], imag.at[1], keep, 512, True)

        def keep_out(columns, value):
            out[:, :, columns] = (trace_first[index, :, :, columns] + halves(value)).astype(BF16)

        spread(middle, direct, crossed)
        product(direct, crossed, real.at[0], imag.at[0], keep_out, 512, True)
        sent[index] = out[...]


def field_kernel(batch, aliased, place_ref, *refs):
    *entries, came, after, constants, real, imag, trace_first, trace_second = refs[: GROUP + 6]
    refs = refs[GROUP + 6 :]
    out, enter, direct, crossed = refs[1:] if aliased else refs
    width = enter.shape[1]
    place = place_ref[0]
    rows = pl.ds(batch * width, width)
    pick_entry(place, 0, entries, came, batch, direct, crossed)

    @pl.when(place != GROUP - 1)
    def _():
        def keep(columns, value):
            enter[:, :, columns] = (halves(value) + constants[batch, :, :, columns].astype(F32)).astype(BF16)

        product(direct, crossed, after.at[0], after.at[1], keep, 512, False)
        spread(enter, direct, crossed)

    def keep_second(columns, value):
        enter[:, :, columns] = (trace_second[batch, :, :, columns] + halves(value)).astype(BF16)

    def keep_first(columns, value):
        out[0, :, rows, columns] = (trace_first[batch, :, :, columns] + halves(value)).astype(BF16)

    product(direct, crossed, real.at[1], imag.at[1], keep_second, 512, True)
    out[1, :, rows, :] = enter[...]
    spread(enter, direct, crossed)
    product(direct, crossed, real.at[0], imag.at[0], keep_first, 512, True)


def shards(source, pivot_inverse_real, factor_imag):
    strips = lax.axis_size(AXIS)
    groups = strips // GROUP
    position = lax.axis_index(AXIS)
    group = position // GROUP
    place = jnp.stack([position % GROUP, group, groups - 1 - group]).astype(jnp.int32)
    size = source.shape[1]
    columns = source.shape[3]
    width = columns // BATCHES
    chunk = columns
    chunks = size // chunk
    total = chunks + 1

    vectors = source.transpose(0, 2, 3, 1)
    real, imag = call(
        stage_kernel,
        tuple(held(*value.shape) for value in (pivot_inverse_real, factor_imag)),
        (pivot_inverse_real, factor_imag),
        [ANY, ANY],
        scratch=[pltpu.SemaphoreType.DMA((2,))],
    )

    nothing = jnp.zeros((2, chunk, size), BF16)
    up = [(s, s + 1) for s in range(strips) if s % GROUP != GROUP - 1]
    down = [(s + 1, s) for s, _ in up]

    def moved(outs, step, pairs, count):
        return lax.ppermute(outs[step - LAG], AXIS, pairs) if 0 <= step < count + LAG * (GROUP - 2) else nothing

    outs_f, outs_b = {}, {}
    kept = ()
    for step in range(-LAG, total + LAG * (GROUP - 2)):
        *kept, outs_f[step], outs_b[step] = sweep(
            step,
            place,
            moved(outs_f, step, up, total),
            moved(outs_b, step, down, chunks),
            real,
            imag,
            vectors,
            kept,
        )
    prefix, prefix_before, suffix, suffix_after = kept

    block = jax.ShapeDtypeStruct((2, width, size), BF16)
    nought = jnp.zeros((2, width, size), BF16)
    block_f = block_i = block_b = nought
    kept_f = kept_i = kept_b = traces = fields = ()
    spread_f, spread_b = {}, {}
    turn = groups - 2
    inner_start = turn + 1
    back_start = inner_start + GROUP - 1
    back_end = back_start + turn
    for moment in range(back_end + BATCHES + 1):
        if moment <= turn + BATCHES:
            kept_f, outgoing, copy = chain(
                moment, turn, False, place, block_f, prefix, vectors, kept_f
            )
            if moment < turn + BATCHES:
                block_f = lax.ppermute(
                    outgoing, AXIS, [(GROUP * g - 1, GROUP * (g + 1) - 1) for g in range(1, groups)]
                )
            if 0 <= moment - turn < BATCHES:
                spread_f[moment - turn] = [
                    lax.ppermute(
                        copy,
                        AXIS,
                        [(GROUP * g + GROUP - 1, GROUP * g + GROUP + other) for g in range(groups - 1)],
                    )
                    for other in range(GROUP - 1)
                ]
        batch = moment - inner_start
        if 0 <= batch < BATCHES:
            outs = [whole(value) for value in traces] or [held(BATCHES, 2, width, size, dtype=F32)] * 2
            traces = call(
                functools.partial(trace_kernel, batch, bool(traces)),
                tuple(outs),
                (
                    place,
                    *spread_f[batch],
                    *map(resident, (kept_f[1], prefix_before, vectors, real, imag, *traces)),
                ),
                [SMEM] + [VMEM] * (GROUP + 4 + len(traces)),
                scratch=[pltpu.VMEM((2, width, size), F32)] + stacked(width, size),
                aliases={GROUP + 5: 0, GROUP + 6: 1} if traces else None,
                times=3,
            )
        if inner_start <= moment < back_start + BATCHES:
            outs = [whole(value) for value in kept_i] or [held(BATCHES, 2, width, size)] * 2
            *kept_i, outgoing = call(
                functools.partial(inner_kernel, moment - inner_start, bool(kept_i)),
                (*outs, block),
                (place, block_i, *map(resident, (real, imag, *traces, *kept_i))),
                [SMEM] + [VMEM] * (5 + len(kept_i)),
                scratch=[pltpu.VMEM((2, width, size), BF16)] + stacked(width, size),
                aliases={6: 0, 7: 1} if kept_i else None,
                times=2,
            )
            if moment < back_start + BATCHES - 1:
                block_i = lax.ppermute(outgoing, AXIS, down)
        if back_start <= moment <= back_end + BATCHES:
            kept_b, outgoing, copy = chain(
                moment - back_start, turn, True, place, block_b, suffix, kept_i[0], kept_b
            )
            if moment < back_end + BATCHES:
                block_b = lax.ppermute(
                    outgoing, AXIS, [(GROUP * g, GROUP * (g - 1)) for g in range(1, groups)]
                )
            if 0 <= moment - back_end < BATCHES:
                spread_b[moment - back_end] = [
                    lax.ppermute(
                        copy,
                        AXIS,
                        [(GROUP * g + GROUP, GROUP * g + other) for g in range(groups - 1)],
                    )
                    for other in range(1, GROUP)
                ]
        batch = moment - back_end - 1
        if batch >= 0:
            fields = (
                call(
                    functools.partial(field_kernel, batch, bool(fields)),
                    whole(fields[0]) if fields else held(2, 2, columns, size),
                    (
                        place,
                        *spread_b[batch],
                        *map(
                            resident,
                            (kept_b[1], suffix_after, kept_i[1], real, imag, *traces, *fields),
                        ),
                    ),
                    [SMEM] + [VMEM] * (GROUP + 6 + len(fields)),
                    scratch=[pltpu.VMEM((2, width, size), BF16)] + stacked(width, size),
                    aliases={GROUP + 7: 0} if fields else None,
                    times=3,
                ),
            )
    return fields[0].transpose(0, 3, 1, 2)


def solution(mesh):
    placed = (P("strip", None, None, "wave"), P("strip", "wave", None), P("strip", "wave", None))
    return jax.shard_map(
        shards,
        mesh=mesh,
        in_specs=placed,
        out_specs=P("strip", None, None, "wave"),
        check_vma=False,
    )
```

```python
import functools

import jax
import jax.numpy as jnp
from jax import lax
from jax.experimental import pallas as pl
from jax.experimental.pallas import tpu as pltpu
from jax.sharding import PartitionSpec as P

GROUP = 4
BATCHES = 4
LAG = 2
AXIS = "strip"
BF16 = jnp.bfloat16
F32 = jnp.float32
MIB = 2**20

VMEM = pl.BlockSpec(memory_space=pltpu.VMEM)
SMEM = pl.BlockSpec(memory_space=pltpu.SMEM)
ANY = pl.BlockSpec(memory_space=pl.ANY)
PLAIN = (((1,), (0,)), ((), ()))
TURNED = (((1,), (1,)), ((), ()))


def resident(value):
    return pltpu.with_memory_space_constraint(value, pltpu.VMEM)


def held(*shape, dtype=BF16):
    return pltpu.VMEM(shape, dtype)


def whole(value):
    return jax.ShapeDtypeStruct(value.shape, value.dtype)


def call(kernel, outs, operands, specs, scratch=(), aliases=None, rows=32, times=1, limit=12):
    size = 1024
    return pl.pallas_call(
        kernel,
        out_shape=outs,
        in_specs=specs,
        out_specs=jax.tree.map(lambda _: VMEM, outs),
        scratch_shapes=scratch,
        input_output_aliases=aliases or {},
        compiler_params=pltpu.CompilerParams(vmem_limit_bytes=limit * MIB),
        cost_estimate=pl.CostEstimate(
            flops=8 * times * rows * size * size, bytes_accessed=4 * times * size * size, transcendentals=0
        ),
    )(*operands)


def product(direct, crossed, real, imag, out, tile, turned):
    dims = TURNED if turned else PLAIN
    tile = min(tile, real.shape[0])

    def body(step, carry):
        columns = pl.ds(pl.multiple_of(step * tile, tile), tile)
        where = (columns, slice(None)) if turned else (slice(None), columns)
        out(
            columns,
            lax.dot_general(direct[...], real[where], dims, preferred_element_type=F32)
            + lax.dot_general(crossed[...], imag[where], dims, preferred_element_type=F32),
        )
        return carry

    lax.fori_loop(0, real.shape[0] // tile, body, 0)


def spread(rows, direct, crossed):
    count = direct.shape[0] // 2
    direct[:count] = rows[0]
    direct[count:] = rows[1]
    crossed[:count] = -rows[1]
    crossed[count:] = rows[0]


def place_in(rows, direct, crossed, columns):
    count = direct.shape[0] // 2
    direct[:count, columns] = rows[0]
    direct[count:, columns] = rows[1]
    crossed[:count, columns] = -rows[1]
    crossed[count:, columns] = rows[0]


def halves(value):
    return value.reshape(2, value.shape[0] // 2, value.shape[1])


def stage_kernel(real, imag, real_out, imag_out, sems):
    copies = [
        pltpu.make_async_copy(real, real_out, sems.at[0]),
        pltpu.make_async_copy(imag, imag_out, sems.at[1]),
    ]
    for copy in copies:
        copy.start()
    for copy in copies:
        copy.wait()


def between(index, count):
    return jnp.logical_and(index >= 0, index < count)


def sweep_kernel(step, aliased, place_ref, block_f, block_b, real, imag, source, *refs):
    own_f, got_f, own_b, got_b, out_f, out_b, direct, crossed, direct_next, crossed_next, result = (
        refs[4:] if aliased else refs
    )
    chunk, size = block_f.shape[1:]
    chunks = size // chunk
    place = place_ref[0]
    index_f = step - LAG * (place - 1)
    index_b = step - LAG * (GROUP - 2 - place)
    last = index_f == chunks
    active_f, active_b = between(index_f, chunks + 1), between(index_b, chunks)
    row_f, row_b = (jnp.clip(index, 0, chunks) * chunk for index in (index_f, index_b))

    for way, (block, row, active, starts) in enumerate(
        (
            (block_f, row_f, active_f, jnp.logical_and(place == 0, jnp.logical_not(last))),
            (block_b, row_b, active_b, place == GROUP - 1),
        )
    ):

        @pl.when(jnp.logical_and(active, starts))
        def _(way=way, row=row):
            shape = (chunk, size)
            hit = lax.broadcasted_iota(jnp.int32, shape, 1) == lax.broadcasted_iota(jnp.int32, shape, 0) + row
            one = jnp.where(hit, 1.0, 0.0).astype(BF16)
            spread((one, jnp.zeros(shape, BF16)), direct.at[way], crossed.at[way])

        @pl.when(jnp.logical_and(active, jnp.logical_not(starts)))
        def _(way=way, block=block):
            spread(block, direct.at[way], crossed.at[way])

    @pl.when(last)
    def _():
        entered = (block_f[...].astype(F32) + source[0].astype(F32)).astype(BF16)
        spread(entered, direct.at[0], crossed.at[0])

    def both(way, carry):
        @pl.when(jnp.logical_or(jnp.logical_and(way == 0, active_f), jnp.logical_and(way == 1, active_b)))
        def _():
            added = jnp.where(jnp.logical_and(way == 0, last), 1.0, 0.0)

            def keep_middle(columns, value):
                place_in(
                    (halves(value) + added * source[1, :, :, columns].astype(F32)).astype(BF16),
                    direct_next,
                    crossed_next,
                    columns,
                )

            def keep(columns, value):
                result[way, :, :, columns] = halves(value).astype(BF16)

            product(direct.at[way], crossed.at[way], real.at[way], imag.at[way], keep_middle, 512, True)
            product(direct_next, crossed_next, real.at[1 - way], imag.at[1 - way], keep, 512, True)

        return carry

    lax.fori_loop(0, 2, both, 0)
    for way, (block, own, got, out, row, active) in enumerate(
        (
            (block_f, own_f, got_f, out_f, row_f, active_f),
            (block_b, own_b, got_b, out_b, row_b, active_b),
        )
    ):

        @pl.when(active)
        def _(way=way, row=row, block=block, own=own, got=got, out=out):
            rows = pl.ds(pl.multiple_of(row, chunk), chunk)
            done = result[way]
            out[...] = done
            own[:, rows, :] = done
            got[:, rows, :] = block[...]


def sweep(step, place, block_f, block_b, real, imag, source, kept):
    _, chunk, size = block_f.shape
    outs = [whole(value) for value in kept] or [
        held(2, length, size) for length in (size + chunk,) * 2 + (size,) * 2
    ]
    return call(
        functools.partial(sweep_kernel, step, bool(kept)),
        (*outs, whole(block_f), whole(block_b)),
        (place, block_f, block_b, resident(real), resident(imag), resident(source), *map(resident, kept)),
        [SMEM] + [VMEM] * (5 + len(kept)),
        scratch=[
            pltpu.VMEM((2, 2 * chunk, size), BF16),
            pltpu.VMEM((2, 2 * chunk, size), BF16),
            pltpu.VMEM((2 * chunk, size), BF16),
            pltpu.VMEM((2 * chunk, size), BF16),
            pltpu.VMEM((2, 2, chunk, size), BF16),
        ],
        aliases={6 + i: i for i in range(4)} if kept else None,
        rows=chunk,
        times=4,
    )


def stacked(count, size):
    return [pltpu.VMEM((2 * count, size), BF16)] * 2


def chain_kernel(moment, spread_from, inward, aliased, place_ref, block, matrix, constants, *refs):
    refs = refs[2:] if aliased else refs
    sent, came, out, copy, direct, crossed = refs
    size = block.shape[2]
    width = block.shape[1]
    place, group, far = place_ref[0], place_ref[1], place_ref[2]
    batch = moment - (far if inward else group)
    node = jnp.logical_and(place == (0 if inward else GROUP - 1), between(batch, BATCHES))
    sends = jnp.logical_and(node, (group if inward else far) > 0)
    index = jnp.clip(batch, 0, BATCHES - 1)

    @pl.when(node)
    def _():
        came[index] = block[...]

    @pl.when(sends)
    def _():
        spread(block, direct, crossed)

        def keep(columns, value):
            if inward:
                constant = constants[index, :, :, columns]
            else:
                constant = matrix[:, pl.ds(pl.multiple_of(size + index * width, width), width), columns]
            out[:, :, columns] = (halves(value) + constant.astype(F32)).astype(BF16)

        product(direct, crossed, matrix.at[0, :size], matrix.at[1, :size], keep, 512, False)
        sent[index] = out[...]

    if 0 <= moment - spread_from < BATCHES:
        copy[...] = sent[moment - spread_from]


def chain(moment, spread_from, inward, place, block, matrix, constants, kept):
    outs = [whole(value) for value in kept] or [held(BATCHES, *block.shape)] * 2
    *kept, out, copy = call(
        functools.partial(chain_kernel, moment, spread_from, inward, bool(kept)),
        (*outs, whole(block), whole(block)),
        (place, block, resident(matrix), resident(constants), *map(resident, kept)),
        [SMEM] + [VMEM] * (3 + len(kept)),
        scratch=stacked(*block.shape[1:]),
        aliases={4: 0, 5: 1} if kept else None,
    )
    return kept, out, copy


def pick_entry(place, mine, entries, came, direct, crossed):
    width = came.shape[2]
    count = BATCHES * width
    others = [other for other in range(GROUP) if other != mine]
    for other, blocks in zip([mine] + others, [[came.at[batch] for batch in range(BATCHES)]] + entries):

        @pl.when(place == other)
        def _(blocks=blocks):
            for batch, block in enumerate(blocks):
                for half in range(2):
                    rows = pl.ds(half * count + batch * width, width)
                    swapped = pl.ds((1 - half) * count + batch * width, width)
                    direct[rows, :] = block[half]
                    crossed[swapped, :] = -block[half] if half else block[half]


def listed(refs):
    return [list(refs[i * BATCHES : (i + 1) * BATCHES]) for i in range(GROUP - 1)]


def trace_kernel(place_ref, *refs):
    passed = (GROUP - 1) * BATCHES
    entries = listed(refs[:passed])
    came, before, source, real, imag, trace_first, trace_second, direct, crossed, enter = refs[passed:]
    size, count = before.shape[2], enter.shape[1]
    place = place_ref[0]
    pick_entry(place, GROUP - 1, entries, came, direct, crossed)

    @pl.when(place == 0)
    def _():
        enter[...] = halves(direct[...]).astype(F32)

    @pl.when(place != 0)
    def _():
        def keep(columns, value):
            enter[:, :, columns] = halves(value) + before[:, pl.ds(size, count), columns].astype(F32)

        product(direct, crossed, before.at[0, :size], before.at[1, :size], keep, 512, False)

    def keep_first(columns, value):
        trace_first[:, :, columns] = halves(value)

    def keep_second(columns, value):
        trace_second[:, :, columns] = halves(value)

    spread((source[0].astype(F32) + enter[...]).astype(BF16), direct, crossed)
    product(direct, crossed, real.at[0], imag.at[0], keep_first, 512, True)
    spread((source[1].astype(F32) + trace_first[...]).astype(BF16), direct, crossed)
    product(direct, crossed, real.at[1], imag.at[1], keep_second, 512, True)


def inner_kernel(moment, aliased, place_ref, block, real, imag, trace_first, trace_second, *refs):
    sent, came, out, middle, direct, crossed = refs[2:] if aliased else refs
    width = block.shape[1]
    mirror = GROUP - 1 - place_ref[0]
    batch = moment - mirror
    index = jnp.clip(batch, 0, BATCHES - 1)
    rows = pl.ds(pl.multiple_of(index * width, width), width)

    @pl.when(between(batch, BATCHES))
    def _():
        middle[...] = trace_second[:, rows, :].astype(BF16)

        @pl.when(mirror != 0)
        def _():
            came[index] = block[...]
            spread(block, direct, crossed)

            def keep(columns, value):
                middle[:, :, columns] = (trace_second[:, rows, columns] + halves(value)).astype(BF16)

            product(direct, crossed, real.at[1], imag.at[1], keep, 512, True)

        def keep_out(columns, value):
            out[:, :, columns] = (trace_first[:, rows, columns] + halves(value)).astype(BF16)

        spread(middle, direct, crossed)
        product(direct, crossed, real.at[0], imag.at[0], keep_out, 512, True)
        sent[index] = out[...]


def field_kernel(place_ref, *refs):
    passed = (GROUP - 1) * BATCHES
    entries = listed(refs[:passed])
    came, after, constants, real, imag, trace_first, trace_second, out, direct, crossed, enter = refs[passed:]
    width = came.shape[2]
    place = place_ref[0]
    pick_entry(place, 0, entries, came, direct, crossed)

    @pl.when(place != GROUP - 1)
    def _():
        def keep(columns, value):
            enter[:, :, columns] = halves(value)

        product(direct, crossed, after.at[0], after.at[1], keep, 512, False)
        for batch in range(BATCHES):
            enter[:, pl.ds(batch * width, width), :] += constants[batch].astype(F32)
        spread(enter[...].astype(BF16), direct, crossed)

    def keep_second(columns, value):
        out[1, :, :, columns] = (trace_second[:, :, columns] + halves(value)).astype(BF16)

    def keep_first(columns, value):
        out[0, :, :, columns] = (trace_first[:, :, columns] + halves(value)).astype(BF16)

    product(direct, crossed, real.at[1], imag.at[1], keep_second, 512, True)
    spread(out.at[1], direct, crossed)
    product(direct, crossed, real.at[0], imag.at[0], keep_first, 512, True)


def shards(source, pivot_inverse_real, factor_imag):
    strips = lax.axis_size(AXIS)
    groups = strips // GROUP
    position = lax.axis_index(AXIS)
    group = position // GROUP
    place = jnp.stack([position % GROUP, group, groups - 1 - group]).astype(jnp.int32)
    size = source.shape[1]
    columns = source.shape[3]
    width = columns // BATCHES
    chunk = columns
    chunks = size // chunk
    total = chunks + 1

    vectors = source.transpose(0, 2, 3, 1)
    real, imag = call(
        stage_kernel,
        tuple(held(*value.shape) for value in (pivot_inverse_real, factor_imag)),
        (pivot_inverse_real, factor_imag),
        [ANY, ANY],
        scratch=[pltpu.SemaphoreType.DMA((2,))],
    )

    nothing = jnp.zeros((2, chunk, size), BF16)
    up = [(s, s + 1) for s in range(strips) if s % GROUP != GROUP - 1]
    down = [(s + 1, s) for s, _ in up]

    def moved(outs, step, pairs, count):
        return lax.ppermute(outs[step - LAG], AXIS, pairs) if 0 <= step < count + LAG * (GROUP - 2) else nothing

    outs_f, outs_b = {}, {}
    kept = ()
    for step in range(-LAG, total + LAG * (GROUP - 2)):
        *kept, outs_f[step], outs_b[step] = sweep(
            step,
            place,
            moved(outs_f, step, up, total),
            moved(outs_b, step, down, chunks),
            real,
            imag,
            vectors,
            kept,
        )
    prefix, prefix_before, suffix, suffix_after = kept

    block = jax.ShapeDtypeStruct((2, width, size), BF16)
    came_f, spread_f = [], []
    hop = jnp.zeros((2, width, size), BF16)
    start = hop
    turn = groups - 2
    kept = ()
    for moment in range(turn + BATCHES + 1):
        kept, outgoing, copy = chain(moment, turn, False, place, hop, prefix, vectors, kept)
        if moment == turn + BATCHES:
            break
        hop = lax.ppermute(
            outgoing,
            AXIS,
            [
                (GROUP * g - 1, GROUP * (g + 1) - 1)
                for g in range(1, groups)
                if 0 <= moment - (g - 1) < BATCHES
            ],
        )
        if moment >= turn:
            spread_f.append(
                [
                    lax.ppermute(
                        copy,
                        AXIS,
                        [(GROUP * g + GROUP - 1, GROUP * g + GROUP + other) for g in range(groups - 1)],
                    )
                    for other in range(GROUP - 1)
                ]
            )

    passed = (GROUP - 1) * BATCHES
    trace = held(2, columns, size, dtype=F32)
    wide = stacked(columns, size) + [pltpu.VMEM((2, columns, size), F32)]
    traces = call(
        trace_kernel,
        (trace, trace),
        (
            place,
            *(blocks[other] for other in range(GROUP - 1) for blocks in spread_f),
            *map(resident, (kept[1], prefix_before, vectors, real, imag)),
        ),
        [SMEM] + [VMEM] * (passed + 5),
        scratch=wide,
        rows=columns,
        times=3,
    )

    spread_b = []
    hop_i = hop_b = start
    kept_i = kept_b = ()
    back_start = GROUP - 1
    back_end = back_start + turn
    for moment in range(back_end + BATCHES + 1):
        if moment < back_start + BATCHES:
            outs = [whole(value) for value in kept_i] or [held(BATCHES, 2, width, size)] * 2
            *kept_i, outgoing = call(
                functools.partial(inner_kernel, moment, bool(kept_i)),
                (*outs, block),
                (place, hop_i, *map(resident, (real, imag, *traces, *kept_i))),
                [SMEM] + [VMEM] * (5 + len(kept_i)),
                scratch=[pltpu.VMEM((2, width, size), BF16)] + stacked(width, size),
                aliases={6: 0, 7: 1} if kept_i else None,
                times=2,
            )
            if moment < back_start + BATCHES - 1:
                hop_i = lax.ppermute(outgoing, AXIS, down)
        if moment >= back_start:
            kept_b, outgoing, copy = chain(
                moment - back_start, turn, True, place, hop_b, suffix, kept_i[0], kept_b
            )
            if moment == back_end + BATCHES:
                break
            hop_b = lax.ppermute(
                outgoing,
                AXIS,
                [
                    (GROUP * g, GROUP * (g - 1))
                    for g in range(1, groups)
                    if 0 <= moment - back_start - (groups - 1 - g) < BATCHES
                ],
            )
            if moment >= back_end:
                spread_b.append(
                    [
                        lax.ppermute(
                            copy,
                            AXIS,
                            [(GROUP * g + GROUP, GROUP * g + other) for g in range(groups - 1)],
                        )
                        for other in range(1, GROUP)
                    ]
                )

    fields = call(
        field_kernel,
        held(2, 2, columns, size),
        (
            place,
            *(blocks[other] for other in range(GROUP - 1) for blocks in spread_b),
            *map(resident, (kept_b[1], suffix_after, kept_i[1], real, imag, *traces)),
        ),
        [SMEM] + [VMEM] * (passed + 7),
        scratch=wide,
        rows=columns,
        times=3,
    )
    return fields.transpose(0, 3, 1, 2)


def solution(mesh):
    placed = (P("strip", None, None, "wave"), P("strip", "wave", None), P("strip", "wave", None))
    return jax.shard_map(
        shards,
        mesh=mesh,
        in_specs=placed,
        out_specs=P("strip", None, None, "wave"),
        check_vma=False,
    )
```

```python
import functools

import jax
import jax.numpy as jnp
from jax import lax
from jax.experimental import pallas as pl
from jax.experimental.pallas import tpu as pltpu
from jax.sharding import PartitionSpec as P

GROUP = 4
BATCHES = 4
STREAMS = 2
LAG = 2
AXIS = "strip"
BF16 = jnp.bfloat16
F32 = jnp.float32
MIB = 2**20

VMEM = pl.BlockSpec(memory_space=pltpu.VMEM)
SMEM = pl.BlockSpec(memory_space=pltpu.SMEM)
ANY = pl.BlockSpec(memory_space=pl.ANY)
PLAIN = (((1,), (0,)), ((), ()))
TURNED = (((1,), (1,)), ((), ()))


def resident(value):
    return pltpu.with_memory_space_constraint(value, pltpu.VMEM)


def held(*shape, dtype=BF16):
    return pltpu.VMEM(shape, dtype)


def whole(value):
    return jax.ShapeDtypeStruct(value.shape, value.dtype)


def call(kernel, outs, operands, specs, scratch=(), aliases=None, rows=32, times=1, limit=12):
    size = 1024
    return pl.pallas_call(
        kernel,
        out_shape=outs,
        in_specs=specs,
        out_specs=jax.tree.map(lambda _: VMEM, outs),
        scratch_shapes=scratch,
        input_output_aliases=aliases or {},
        compiler_params=pltpu.CompilerParams(vmem_limit_bytes=limit * MIB),
        cost_estimate=pl.CostEstimate(
            flops=8 * times * rows * size * size, bytes_accessed=4 * times * size * size, transcendentals=0
        ),
    )(*operands)


def product(direct, crossed, real, imag, out, tile, turned):
    dims = TURNED if turned else PLAIN
    tile = min(tile, real.shape[0])

    def body(step, carry):
        columns = pl.ds(pl.multiple_of(step * tile, tile), tile)
        where = (columns, slice(None)) if turned else (slice(None), columns)
        out(
            columns,
            lax.dot_general(direct[...], real[where], dims, preferred_element_type=F32)
            + lax.dot_general(crossed[...], imag[where], dims, preferred_element_type=F32),
        )
        return carry

    lax.fori_loop(0, real.shape[0] // tile, body, 0)


def spread(rows, direct, crossed):
    count = direct.shape[0] // 2
    direct[:count] = rows[0]
    direct[count:] = rows[1]
    crossed[:count] = -rows[1]
    crossed[count:] = rows[0]


def place_in(rows, direct, crossed, columns):
    count = direct.shape[0] // 2
    direct[:count, columns] = rows[0]
    direct[count:, columns] = rows[1]
    crossed[:count, columns] = -rows[1]
    crossed[count:, columns] = rows[0]


def halves(value):
    return value.reshape(2, value.shape[0] // 2, value.shape[1])


def stage_kernel(real, imag, real_out, imag_out, sems):
    copies = [
        pltpu.make_async_copy(real, real_out, sems.at[0]),
        pltpu.make_async_copy(imag, imag_out, sems.at[1]),
    ]
    for copy in copies:
        copy.start()
    for copy in copies:
        copy.wait()


def between(index, count):
    return jnp.logical_and(index >= 0, index < count)


def sweep_kernel(step, aliased, place_ref, block_f, block_b, real, imag, source, *refs):
    own_f, got_f, own_b, got_b, out_f, out_b, direct, crossed, direct_next, crossed_next, result = (
        refs[4:] if aliased else refs
    )
    chunk, size = block_f.shape[1:]
    chunks = size // chunk
    place = place_ref[0]
    index_f = step - LAG * (place - 1)
    index_b = step - LAG * (GROUP - 2 - place)
    vector = index_f == 0
    active_f, active_b = between(index_f, chunks + 1), between(index_b, chunks)
    row_f = jnp.where(vector, chunks, jnp.clip(index_f - 1, 0, chunks)) * chunk
    row_b = jnp.clip(index_b, 0, chunks) * chunk

    for way, (block, row, active, starts) in enumerate(
        (
            (block_f, row_f, active_f, jnp.logical_and(place == 0, jnp.logical_not(vector))),
            (block_b, row_b, active_b, place == GROUP - 1),
        )
    ):

        @pl.when(jnp.logical_and(active, starts))
        def _(way=way, row=row):
            shape = (chunk, size)
            hit = lax.broadcasted_iota(jnp.int32, shape, 1) == lax.broadcasted_iota(jnp.int32, shape, 0) + row
            one = jnp.where(hit, 1.0, 0.0).astype(BF16)
            spread((one, jnp.zeros(shape, BF16)), direct.at[way], crossed.at[way])

        @pl.when(jnp.logical_and(active, jnp.logical_not(starts)))
        def _(way=way, block=block):
            spread(block, direct.at[way], crossed.at[way])

    @pl.when(vector)
    def _():
        entered = (block_f[...].astype(F32) + source[0].astype(F32)).astype(BF16)
        spread(entered, direct.at[0], crossed.at[0])

    def both(way, carry):
        @pl.when(jnp.logical_or(jnp.logical_and(way == 0, active_f), jnp.logical_and(way == 1, active_b)))
        def _():
            added = jnp.where(jnp.logical_and(way == 0, vector), 1.0, 0.0)

            def keep_middle(columns, value):
                place_in(
                    (halves(value) + added * source[1, :, :, columns].astype(F32)).astype(BF16),
                    direct_next,
                    crossed_next,
                    columns,
                )

            def keep(columns, value):
                result[way, :, :, columns] = halves(value).astype(BF16)

            product(direct.at[way], crossed.at[way], real.at[way], imag.at[way], keep_middle, 1024, True)
            product(direct_next, crossed_next, real.at[1 - way], imag.at[1 - way], keep, 1024, True)

        return carry

    lax.fori_loop(0, 2, both, 0)
    for way, (block, own, got, out, row, active) in enumerate(
        (
            (block_f, own_f, got_f, out_f, row_f, active_f),
            (block_b, own_b, got_b, out_b, row_b, active_b),
        )
    ):

        @pl.when(active)
        def _(way=way, row=row, block=block, own=own, got=got, out=out):
            rows = pl.ds(pl.multiple_of(row, chunk), chunk)
            done = result[way]
            out[...] = done
            own[:, rows, :] = done
            got[:, rows, :] = block[...]


def sweep(step, place, block_f, block_b, real, imag, source, kept):
    _, chunk, size = block_f.shape
    outs = [whole(value) for value in kept] or [
        held(2, length, size) for length in (size + chunk,) * 2 + (size,) * 2
    ]
    return call(
        functools.partial(sweep_kernel, step, bool(kept)),
        (*outs, whole(block_f), whole(block_b)),
        (place, block_f, block_b, resident(real), resident(imag), resident(source), *map(resident, kept)),
        [SMEM] + [VMEM] * (5 + len(kept)),
        scratch=[
            pltpu.VMEM((2, 2 * chunk, size), BF16),
            pltpu.VMEM((2, 2 * chunk, size), BF16),
            pltpu.VMEM((2 * chunk, size), BF16),
            pltpu.VMEM((2 * chunk, size), BF16),
            pltpu.VMEM((2, 2, chunk, size), BF16),
        ],
        aliases={6 + i: i for i in range(4)} if kept else None,
        rows=chunk,
        times=4,
    )


def stacked(count, size):
    return [pltpu.VMEM((2 * count, size), BF16)] * 2


def chain_kernel(
    moment, stream, spread_from, inward, aliased, place_ref, block, matrix, constants, *refs
):
    refs = refs[2:] if aliased else refs
    sent, came, out, copy, direct, crossed = refs
    size = block.shape[2]
    width = block.shape[1]
    place, group, far = place_ref[0], place_ref[1], place_ref[2]
    step = moment - (far if inward else group - 1)
    node = jnp.logical_and(place == (0 if inward else GROUP - 1), between(step, BATCHES // STREAMS))
    index = jnp.clip(step, 0, BATCHES // STREAMS - 1) * STREAMS + stream
    rows = pl.ds(pl.multiple_of(index * width, width), width)
    own = pl.ds(pl.multiple_of(size + index * width, width), width)

    @pl.when(node)
    def _():
        if inward:
            came[index] = block[...]
        else:
            @pl.when(group == 1)
            def _():
                came[index] = constants[:, rows, :]

            @pl.when(group != 1)
            def _():
                came[index] = block[...]

    sends = jnp.logical_and(node, (group if inward else far) > 0)
    if inward:
        @pl.when(jnp.logical_and(sends, far == 0))
        def _():
            out[...] = constants[index]
            sent[index] = out[...]

        sends = jnp.logical_and(sends, far > 0)

    @pl.when(sends)
    def _():
        spread(came.at[index], direct, crossed)

        def keep(columns, value):
            constant = constants[index, :, :, columns] if inward else matrix[:, own, columns]
            out[:, :, columns] = (halves(value) + constant.astype(F32)).astype(BF16)

        product(direct, crossed, matrix.at[0, :size], matrix.at[1, :size], keep, 512, False)
        sent[index] = out[...]

    batch = (moment - spread_from) * STREAMS
    if stream == STREAMS - 1 and 0 <= batch < BATCHES:
        if inward:
            copy[...] = sent[batch : batch + STREAMS]
        else:
            @pl.when(group == 0)
            def _():
                for other in range(STREAMS):
                    copy[other] = matrix[:, pl.ds(size + (batch + other) * width, width), :]

            @pl.when(group != 0)
            def _():
                copy[...] = sent[batch : batch + STREAMS]


def chain(moment, stream, spread_from, inward, place, block, matrix, constants, kept):
    outs = [whole(value) for value in kept] or [held(BATCHES, *block.shape)] * 2
    *kept, out, copy = call(
        functools.partial(chain_kernel, moment, stream, spread_from, inward, bool(kept)),
        (*outs, whole(block), jax.ShapeDtypeStruct((STREAMS, *block.shape), BF16)),
        (place, block, resident(matrix), resident(constants), *map(resident, kept)),
        [SMEM] + [VMEM] * (3 + len(kept)),
        scratch=stacked(*block.shape[1:]),
        aliases={4: 0, 5: 1} if kept else None,
    )
    return kept, out, copy


def pick_entry(place, mine, entries, came, direct, crossed):
    width = came.shape[2]
    count = BATCHES * width
    others = [other for other in range(GROUP) if other != mine]
    for other, blocks in zip([mine] + others, [[came.at[batch] for batch in range(BATCHES)]] + entries):

        @pl.when(place == other)
        def _(blocks=blocks):
            for batch in range(BATCHES):
                block = blocks[batch]
                for half in range(2):
                    rows = pl.ds(half * count + batch * width, width)
                    swapped = pl.ds((1 - half) * count + batch * width, width)
                    direct[rows, :] = block[half]
                    crossed[swapped, :] = -block[half] if half else block[half]


def listed(refs):
    depth = BATCHES // STREAMS
    return [
        [ref.at[stream] for ref in refs[i * depth : (i + 1) * depth] for stream in range(STREAMS)]
        for i in range(GROUP - 1)
    ]


def trace_kernel(place_ref, *refs):
    passed = (GROUP - 1) * (BATCHES // STREAMS)
    entries = listed(refs[:passed])
    came, before, source, real, imag, trace_first, trace_second, direct, crossed, enter = refs[passed:]
    size, count = before.shape[2], enter.shape[1]
    place = place_ref[0]
    pick_entry(place, GROUP - 1, entries, came, direct, crossed)

    @pl.when(place == 0)
    def _():
        enter[...] = halves(direct[...]).astype(F32)

    @pl.when(place != 0)
    def _():
        def keep(columns, value):
            enter[:, :, columns] = halves(value) + before[:, pl.ds(size, count), columns].astype(F32)

        product(direct, crossed, before.at[0, :size], before.at[1, :size], keep, 512, False)

    def keep_first(columns, value):
        trace_first[:, :, columns] = halves(value)

    def keep_second(columns, value):
        trace_second[:, :, columns] = halves(value)

    spread((source[0].astype(F32) + enter[...]).astype(BF16), direct, crossed)
    product(direct, crossed, real.at[0], imag.at[0], keep_first, 512, True)
    spread((source[1].astype(F32) + trace_first[...]).astype(BF16), direct, crossed)
    product(direct, crossed, real.at[1], imag.at[1], keep_second, 512, True)


def inner_kernel(moment, stream, aliased, place_ref, block, real, imag, trace_first, trace_second, *refs):
    sent, came, out, middle, direct, crossed = refs[2:] if aliased else refs
    width = block.shape[1]
    mirror = GROUP - 1 - place_ref[0]
    step = moment - mirror
    index = jnp.clip(step, 0, BATCHES // STREAMS - 1) * STREAMS + stream
    rows = pl.ds(pl.multiple_of(index * width, width), width)

    @pl.when(between(step, BATCHES // STREAMS))
    def _():
        middle[...] = trace_second[:, rows, :].astype(BF16)

        @pl.when(mirror != 0)
        def _():
            came[index] = block[...]
            spread(block, direct, crossed)

            def keep(columns, value):
                middle[:, :, columns] = (trace_second[:, rows, columns] + halves(value)).astype(BF16)

            product(direct, crossed, real.at[1], imag.at[1], keep, 512, True)

        def keep_out(columns, value):
            out[:, :, columns] = (trace_first[:, rows, columns] + halves(value)).astype(BF16)

        spread(middle, direct, crossed)
        product(direct, crossed, real.at[0], imag.at[0], keep_out, 512, True)
        sent[index] = out[...]


def field_kernel(place_ref, *refs):
    passed = (GROUP - 1) * (BATCHES // STREAMS)
    entries = listed(refs[:passed])
    came, after, constants, real, imag, trace_first, trace_second, out, direct, crossed, enter = refs[passed:]
    width = came.shape[2]
    place = place_ref[0]
    pick_entry(place, 0, entries, came, direct, crossed)

    @pl.when(place != GROUP - 1)
    def _():
        def keep(columns, value):
            enter[:, :, columns] = halves(value)

        product(direct, crossed, after.at[0], after.at[1], keep, 512, False)
        for batch in range(BATCHES):
            enter[:, pl.ds(batch * width, width), :] += constants[batch].astype(F32)
        spread(enter[...].astype(BF16), direct, crossed)

    def keep_second(columns, value):
        out[1, :, :, columns] = (trace_second[:, :, columns] + halves(value)).astype(BF16)

    def keep_first(columns, value):
        out[0, :, :, columns] = (trace_first[:, :, columns] + halves(value)).astype(BF16)

    product(direct, crossed, real.at[1], imag.at[1], keep_second, 512, True)
    spread(out.at[1], direct, crossed)
    product(direct, crossed, real.at[0], imag.at[0], keep_first, 512, True)


def shards(source, pivot_inverse_real, factor_imag):
    strips = lax.axis_size(AXIS)
    groups = strips // GROUP
    position = lax.axis_index(AXIS)
    group = position // GROUP
    place = jnp.stack([position % GROUP, group, groups - 1 - group]).astype(jnp.int32)
    size = source.shape[1]
    columns = source.shape[3]
    width = columns // BATCHES
    chunk = columns
    chunks = size // chunk
    total = chunks + 1

    vectors = source.transpose(0, 2, 3, 1)
    real, imag = call(
        stage_kernel,
        tuple(held(*value.shape) for value in (pivot_inverse_real, factor_imag)),
        (pivot_inverse_real, factor_imag),
        [ANY, ANY],
        scratch=[pltpu.SemaphoreType.DMA((2,))],
    )

    nothing = jnp.zeros((2, chunk, size), BF16)
    up = [(s, s + 1) for s in range(strips) if s % GROUP != GROUP - 1]
    down = [(s + 1, s) for s, _ in up]

    def moved(outs, step, pairs, count):
        return lax.ppermute(outs[step - LAG], AXIS, pairs) if 0 <= step < count + LAG * (GROUP - 2) else nothing

    outs_f, outs_b = {}, {}
    kept = ()
    for step in range(-LAG, total + LAG * (GROUP - 2)):
        *kept, outs_f[step], outs_b[step] = sweep(
            step,
            place,
            moved(outs_f, step, up, total),
            moved(outs_b, step, down, chunks),
            real,
            imag,
            vectors,
            kept,
        )
        if step == LAG * (GROUP - 2):
            head = lax.ppermute(outs_f[step], AXIS, [(GROUP - 1, 2 * GROUP - 1)])
    prefix, prefix_before, suffix, suffix_after = kept

    block = jax.ShapeDtypeStruct((2, width, size), BF16)
    spread_f = []
    start = jnp.zeros((2, width, size), BF16)
    hops = [start] * STREAMS
    turn = groups - 3
    kept = ()
    depth = BATCHES // STREAMS
    forth = [(GROUP * g - 1, GROUP * (g + 1) - 1) for g in range(1, groups)]
    back = [(d - GROUP + 1, s - GROUP + 1) for s, d in reversed(forth)]
    half = groups // 2 - 1

    def reach(pairs, moment):
        return pairs[:half] if moment + 1 <= half else pairs[half - depth + 1 :]

    for moment in range(turn + depth + 1):
        for stream in range(STREAMS):
            kept, outgoing, copy = chain(
                moment, stream, turn, False, place, hops[stream], prefix, head, kept
            )
            if moment < turn + depth:
                hops[stream] = lax.ppermute(outgoing, AXIS, reach(forth[1:], moment))
            if stream == STREAMS - 1 and turn <= moment < turn + depth:
                spread_f.append(
                    [
                        lax.ppermute(copy, AXIS, [(s, d - GROUP + 1 + other) for s, d in forth])
                        for other in range(GROUP - 1)
                    ]
                )

    passed = (GROUP - 1) * (BATCHES // STREAMS)
    trace = held(2, columns, size, dtype=F32)
    wide = stacked(columns, size) + [pltpu.VMEM((2, columns, size), F32)]
    traces = call(
        trace_kernel,
        (trace, trace),
        (
            place,
            *(blocks[other] for other in range(GROUP - 1) for blocks in spread_f),
            *map(resident, (kept[1], prefix_before, vectors, real, imag)),
        ),
        [SMEM] + [VMEM] * (passed + 5),
        scratch=wide,
        rows=columns,
        times=3,
    )

    spread_b = []
    hops_i, hops_b = [start] * STREAMS, [start] * STREAMS
    kept_i = kept_b = ()
    turn = groups - 2
    for moment in range(GROUP - 1 + turn + depth + 1):
        beyond = moment - GROUP + 1
        for stream in range(STREAMS):
            if beyond < depth:
                outs = [whole(value) for value in kept_i] or [held(BATCHES, 2, width, size)] * 2
                *kept_i, outgoing = call(
                    functools.partial(inner_kernel, moment, stream, bool(kept_i)),
                    (*outs, block),
                    (place, hops_i[stream], *map(resident, (real, imag, *traces, *kept_i))),
                    [SMEM] + [VMEM] * (5 + len(kept_i)),
                    scratch=[pltpu.VMEM((2, width, size), BF16)] + stacked(width, size),
                    aliases={6: 0, 7: 1} if kept_i else None,
                    times=2,
                )
                if beyond < depth - 1:
                    hops_i[stream] = lax.ppermute(outgoing, AXIS, down)
            if beyond >= 0:
                kept_b, outgoing, copy = chain(
                    beyond, stream, turn, True, place, hops_b[stream], suffix, kept_i[0], kept_b
                )
                if beyond < turn + depth:
                    hops_b[stream] = lax.ppermute(outgoing, AXIS, reach(back, beyond))
                if stream == STREAMS - 1 and turn <= beyond < turn + depth:
                    spread_b.append(
                        [
                            lax.ppermute(copy, AXIS, [(s, d + other) for s, d in back])
                            for other in range(1, GROUP)
                        ]
                    )

    fields = call(
        field_kernel,
        held(2, 2, columns, size),
        (
            place,
            *(blocks[other] for other in range(GROUP - 1) for blocks in spread_b),
            *map(resident, (kept_b[1], suffix_after, kept_i[1], real, imag, *traces)),
        ),
        [SMEM] + [VMEM] * (passed + 7),
        scratch=wide,
        rows=columns,
        times=3,
    )
    return fields.transpose(0, 3, 1, 2)


def solution(mesh):
    placed = (P("strip", None, None, "wave"), P("strip", "wave", None), P("strip", "wave", None))
    return jax.shard_map(
        shards,
        mesh=mesh,
        in_specs=placed,
        out_specs=P("strip", None, None, "wave"),
        check_vma=False,
    )
```
